32 devices in a mesh: seq: 8 (over y, x, core), head: 4 (over z).
Axes of the slice: x: 2, y: 2, z: 4, core: 2. Of those that a mesh axis runs over, the one named last changes fastest.
Arguments:
- inputs: bfloat16 [2048, 4096], P('seq', 'head'), may hold values from -6 to 6
- gates: bfloat16 [2048, 4096], P('seq', 'head'), may hold values from -6 to 6
- b_proj: bfloat16 [2048, 128], P('seq'), may hold values from -6 to 6
- c_proj: bfloat16 [2048, 128], P('seq'), may hold values from -6 to 6
- step_size: float32 [64, 2048], P('head', 'seq'), may hold values from 0 to 2
- decay_rate: float32 [64], P('head'), may hold values from 0.5 to 2
- norm_gain: float32 [4096], P('head'), may hold values from 0.5 to 1.5
- out_weight: bfloat16 [4096, 4096], P('seq', 'head'), may hold values from -0.09375 to 0.09375
- grad_out: bfloat16 [2048, 4096], P('seq', 'head'), may hold values from -6 to 6
Outputs:
- grad_inputs: bfloat16 [2048, 4096], P('seq', 'head')
- grad_gates: bfloat16 [2048, 4096], P('seq', 'head')
- grad_b: float32 [2048, 128], P('seq')
- grad_c: float32 [2048, 128], P('seq')
- grad_step: float32 [64, 2048], P('head', 'seq')
- grad_rate: float32 [64], P('head')
- grad_gain: float32 [4096], P('head')
- grad_weight: float32 [4096, 4096], P('seq', 'head')
The draws below stay inside these ranges and needn't reach their ends.
All inputs are finite; a program needn't handle non-finite values.
Results may differ from the reference program's by a relative error of at most 0.0042.
Values may be sent and summed in bfloat16 or wider, within the bound.
No kernel may reach another device: no remote copies, remote signals or barrier semaphores. Data moves between devices by JAX's collectives and lax.ppermute only.
A program may use at most 64 MiB of HBM per device.

```python
import jax
import jax.numpy as jnp
from jax import lax

D = 4096
HEADS = 64
HEAD_DIM = 64
STATE = 128
TOK_DEV = 256
STREAM_WORDS = 2048
N_SEQ = 8


def rates_and_steps(key):
    stochastic_seeds = jax.random.split(jax.random.fold_in(key, 11), 8)
    rate = jnp.exp(jax.random.uniform(stochastic_seeds[0], (HEADS,), jnp.float32, jnp.log(0.5), jnp.log(2.0)))
    share = 0.5
    quick = jax.random.uniform(stochastic_seeds[1], (HEADS,), jnp.float32) < share
    quick_step = jax.random.uniform(stochastic_seeds[2], (HEADS,), jnp.float32, 1.0 / 50.0, 1.0 / 30.0)
    slow_step = jax.random.uniform(stochastic_seeds[3], (HEADS,), jnp.float32, 0.1, 0.5) / STREAM_WORDS
    single_update_expense = jnp.where(quick, quick_step, slow_step)
    blocks = STREAM_WORDS // TOK_DEV
    tile_factor = jnp.exp(jax.random.uniform(stochastic_seeds[4], (HEADS, blocks), jnp.float32, jnp.log(0.5), jnp.log(2.0)))
    tile_factor = jnp.repeat(tile_factor, TOK_DEV, axis=1)
    approximate_guess = jax.random.uniform(stochastic_seeds[5], (HEADS, STREAM_WORDS), jnp.float32, 0.5, 1.5)
    span_extent = jax.random.uniform(stochastic_seeds[6], (STREAM_WORDS,), jnp.float32) < 3.0 / STREAM_WORDS
    objective_number = jax.random.uniform(stochastic_seeds[7], (HEADS, STREAM_WORDS), jnp.float32, 0.22, 0.69)
    overall_tally = single_update_expense[:, None] * tile_factor * approximate_guess + jnp.where(span_extent[None, :], objective_number, 0.0)
    return (rate, overall_tally / rate[:, None])


def draw_decay_rate(key, part):
    return rates_and_steps(key)[0]


def draw_step_size(key, part):
    return rates_and_steps(key)[1]


def with_spikes(result, key, source, target, blocks, factor):
    owner, partner = [(jnp.arange(result.shape[axis_at]) // (result.shape[axis_at] // blocks)).reshape([-1 if axis == axis_at else 1 for axis in range(result.ndim)]) for axis_at in (source, target)]
    chosen = jax.random.permutation(key, blocks)[partner]
    strong = (owner == chosen) | (owner == (partner + blocks // 2) % blocks)
    return jnp.where(strong, factor * result, result)


def shard_levels(rng, dims, pieces, least, high):
    def one(dim, blocks):
        heights = jax.random.uniform(jax.random.fold_in(jax.random.fold_in(rng, 6), dim), (blocks,), jnp.float32, least / len(pieces), high / len(pieces))
        return jnp.repeat(jnp.exp(heights), dims[dim] // blocks).reshape((-1,) + (1,) * (len(dims) - dim - 1))

    loudness = one(*pieces[0])
    for cut in pieces[1:]:
        loudness = loudness * one(*cut)
    return loudness


def centred(stream_key, extent, deviation, bound, shards=(), held_as=jnp.bfloat16):
    drawn = jax.random.normal(stream_key, extent, jnp.float32) * deviation
    if len(shards) > 0:
        drawn = shard_levels(stream_key, extent, shards, -0.22, 0.18) * drawn
    return jnp.clip(drawn, min=-bound, max=bound).astype(held_as)


def heavy_noise(stream_key, extent, deviation, reach, pieces, heavy, dtype=jnp.bfloat16):
    drawn = deviation * jax.random.normal(stream_key, extent, jnp.float32)
    if pieces:
        drawn = drawn * shard_levels(stream_key, extent, pieces, -0.22, 0.18)
    return jnp.clip(with_spikes(drawn, jax.random.fold_in(stream_key, 3), *heavy), -reach, reach).astype(dtype)


def setup_inputs(seed: int = 0) -> dict:
    key_list = jax.random.split(jax.random.key(seed), 10)
    return {
        "inputs": centred(key_list[0], (STREAM_WORDS, HEADS * HEAD_DIM), 1.0, 6.0, ((0, 8), (1, 4))),
        "gates": centred(key_list[1], (STREAM_WORDS, HEADS * HEAD_DIM), 1.0, 6.0, ((0, 8), (1, 4))),
        "b_proj": centred(key_list[2], (STREAM_WORDS, STATE), 1.0, 6.0, ((0, 8),)),
        "c_proj": centred(key_list[3], (STREAM_WORDS, STATE), 1.0, 6.0, ((0, 8),)),
        "step_size": draw_step_size(jax.random.fold_in(key_list[9], 71), 0),
        "decay_rate": draw_decay_rate(jax.random.fold_in(key_list[9], 71), 0),
        "norm_gain": jnp.clip(1.0 + 0.1 * jax.random.normal(key_list[6], (HEADS * HEAD_DIM,), jnp.float32), 0.5, 1.5),
        "out_weight": centred(key_list[7], (D, HEADS * HEAD_DIM), (HEADS * HEAD_DIM) ** -0.5, 0.09375, ((0, 8), (1, 4))),
        "grad_out": heavy_noise(key_list[8], (STREAM_WORDS, D), 1.0, 6.0, ((0, 8), (1, 4)), (0, 1, 8, 2.0)),
    }


EPSILON = 1e-05

def dot_high(left, right):
    return jnp.dot(left, right, precision=lax.Precision.HIGHEST, preferred_element_type=jnp.float32)

def dot_inner(left, right):
    return lax.dot_general(left, right, (((0,), (0,)), ((), ())), precision=lax.Precision.HIGHEST, preferred_element_type=jnp.float32)

def decay_table(step, rate):
    logs = -jnp.cumsum(rate * step)
    count = step.shape[0]
    later = lax.broadcasted_iota(jnp.int32, (count, count), 0)
    earlier = lax.broadcasted_iota(jnp.int32, (count, count), 1)
    spread = jnp.minimum(logs[:, None] - logs[None, :], 0.0)
    table = jnp.where(later >= earlier, jnp.exp(spread), 0.0)
    return (logs, table)

def span_summary(step, rate, values, keys_b):
    logs = -jnp.cumsum(rate * step)
    tail = jnp.exp(logs[-1] - logs)
    return (jnp.exp(logs[-1]), dot_inner(keys_b * (step * tail)[:, None], values))

def span_output(step, rate, values, keys_b, queries_c, state_in):
    logs, table = decay_table(step, rate)
    scores = dot_high(queries_c, keys_b.T)
    mixing = table * scores * step[None, :]
    return dot_high(mixing, values) + jnp.exp(logs)[:, None] * dot_high(queries_c, state_in)

def adjoint_summary(step, rate, queries_c, grads):
    logs = -jnp.cumsum(rate * step)
    return (jnp.exp(logs[-1]), dot_inner(queries_c * jnp.exp(logs)[:, None], grads))

def span_backward(step, rate, values, keys_b, queries_c, grads, state_in, adjoint_in):
    logs, table = decay_table(step, rate)
    tail = jnp.exp(logs[-1] - logs)
    front = jnp.exp(logs)
    scores = dot_high(queries_c, keys_b.T)
    inner = dot_high(grads, values.T)
    weighted = table * inner
    mixing = table * scores * step[None, :]
    keys_adjoint = dot_high(keys_b, adjoint_in)
    grad_values = dot_inner(mixing, grads) + (step * tail)[:, None] * keys_adjoint
    grad_keys = step[:, None] * (dot_inner(weighted, queries_c) + tail[:, None] * dot_high(values, adjoint_in.T))
    grad_queries = dot_high(weighted * step[None, :], keys_b) + front[:, None] * dot_high(grads, state_in.T)
    carried = tail * lax.optimization_barrier(jnp.sum(keys_adjoint * values, axis=1))
    q_terms = lax.optimization_barrier(jnp.sum(weighted * scores, axis=0)) + carried
    row_part = lax.optimization_barrier(jnp.sum(mixing * inner, axis=1)) + front * lax.optimization_barrier(jnp.sum(dot_high(queries_c, state_in) * grads, axis=1))
    drive = row_part - step * q_terms
    state_end = jnp.exp(logs[-1]) * state_in + dot_inner(keys_b * (step * tail)[:, None], values)
    boundary = jnp.sum(adjoint_in * state_end)
    log_grad = jnp.flip(jnp.cumsum(jnp.flip(drive))) + boundary
    grad_step = q_terms - rate * log_grad
    rate_part = -jnp.sum(step * log_grad)
    return (grad_values, grad_keys, grad_queries, grad_step, rate_part)

def reference(inputs, gates, b_proj, c_proj, step_size, decay_rate, norm_gain, out_weight, grad_out):
    spans = N_SEQ
    length = TOK_DEV
    width = HEADS * HEAD_DIM
    grad_normed = jnp.dot(grad_out, out_weight, preferred_element_type=jnp.float32)
    values = inputs.astype(jnp.float32).reshape(spans, length, HEADS, HEAD_DIM).transpose(0, 2, 1, 3)
    keys_b = b_proj.astype(jnp.float32).reshape(spans, length, STATE)
    queries_c = c_proj.astype(jnp.float32).reshape(spans, length, STATE)
    steps = step_size.reshape(HEADS, spans, length).transpose(1, 0, 2)

    def forward_step(state, items):
        span_values, span_keys, span_queries, span_steps = items
        outputs = jax.vmap(span_output, in_axes=(0, 0, 0, None, None, 0))(span_steps, decay_rate, span_values, span_keys, span_queries, state)
        decays, local = jax.vmap(span_summary, in_axes=(0, 0, 0, None))(span_steps, decay_rate, span_values, span_keys)
        return (decays[:, None, None] * state + local, (outputs, state))
    start = jnp.zeros((HEADS, STATE, HEAD_DIM), jnp.float32)
    _, (outputs, states_in) = lax.scan(forward_step, start, (values, keys_b, queries_c, steps))
    ssd_out = outputs.transpose(0, 2, 1, 3).reshape(STREAM_WORDS, width)
    gate_values = gates.astype(jnp.float32)
    sigmoid_gate = jax.nn.sigmoid(gate_values)
    gated = ssd_out * gate_values * sigmoid_gate
    inv_rms = lax.rsqrt(lax.optimization_barrier(jnp.mean(gated * gated, axis=1)) + EPSILON)
    normed = (gated * inv_rms[:, None] * norm_gain[None, :]).astype(jnp.bfloat16)
    grad_weight = lax.dot_general(grad_out, normed, (((0,), (0,)), ((), ())), preferred_element_type=jnp.float32)
    grad_gain = lax.optimization_barrier(jnp.sum(grad_normed * gated * inv_rms[:, None], axis=0))
    scaled = grad_normed * norm_gain[None, :]
    cross_mean = lax.optimization_barrier(jnp.mean(scaled * gated, axis=1))
    grad_gated = inv_rms[:, None] * (scaled - gated * (inv_rms * inv_rms * cross_mean)[:, None])
    grad_ssd = grad_gated * gate_values * sigmoid_gate
    grad_gates = (grad_gated * ssd_out * sigmoid_gate * (1.0 + gate_values * (1.0 - sigmoid_gate))).astype(jnp.bfloat16)
    grads = grad_ssd.reshape(spans, length, HEADS, HEAD_DIM).transpose(0, 2, 1, 3)

    def backward_step(adjoint, items):
        span_values, span_keys, span_queries, span_steps, span_grads, state_in = items
        parts = jax.vmap(span_backward, in_axes=(0, 0, 0, None, None, 0, 0, 0))(span_steps, decay_rate, span_values, span_keys, span_queries, span_grads, state_in, adjoint)
        decays, local = jax.vmap(adjoint_summary, in_axes=(0, 0, None, 0))(span_steps, decay_rate, span_queries, span_grads)
        return (local + decays[:, None, None] * adjoint, parts)
    _, parts = lax.scan(backward_step, start, (values, keys_b, queries_c, steps, grads, states_in), reverse=True)
    grad_values, grad_keys, grad_queries, grad_steps, rate_parts = parts
    grad_inputs = grad_values.transpose(0, 2, 1, 3).reshape(STREAM_WORDS, width).astype(jnp.bfloat16)
    grad_b = lax.optimization_barrier(jnp.sum(grad_keys, axis=1)).reshape(STREAM_WORDS, STATE)
    grad_c = lax.optimization_barrier(jnp.sum(grad_queries, axis=1)).reshape(STREAM_WORDS, STATE)
    grad_step = grad_steps.transpose(1, 0, 2).reshape(HEADS, STREAM_WORDS)
    grad_rate = lax.optimization_barrier(jnp.sum(rate_parts, axis=0))
    return (grad_inputs, grad_gates, grad_b, grad_c, grad_step, grad_rate, grad_gain, grad_weight)
```

```python
import functools

import jax
import jax.numpy as jnp
from jax import lax
from jax.experimental import pallas as pl
from jax.experimental.pallas import tpu as pltpu
from jax.sharding import PartitionSpec as P

EPSILON = 1e-05
F32 = jnp.float32
BF16 = jnp.bfloat16
LANES = 128
ROWS = 8
NN = ((1,), (0,))
NT = ((1,), (1,))
TN = ((0,), (0,))
HIGHEST = lax.Precision.HIGHEST


def mm(left, right, dims):
    return lax.dot_general(left, right, (dims, ((), ())), preferred_element_type=F32)


def mm_f32(left, right, dims):
    return lax.dot_general(
        left, right, (dims, ((), ())), precision=HIGHEST, preferred_element_type=F32
    )


def two(value):
    high = value.astype(BF16)
    return high, (value - high.astype(F32)).astype(BF16)


def three(value):
    high = value.astype(BF16)
    rest = value - high.astype(F32)
    middle = rest.astype(BF16)
    return high, middle, (rest - middle.astype(F32)).astype(BF16)


def mm_exact_left(left, right, dims):
    high, low = two(right)
    return mm(left, high, dims) + mm(left, low, dims)


def mm_exact_right(left, right, dims):
    high, low = two(left)
    return mm(high, right, dims) + mm(low, right, dims)


def mm_both(left, right, dims):
    left_high, left_low = two(left)
    right_high, right_low = two(right)
    return (
        mm(left_high, right_high, dims)
        + mm(left_low, right_high, dims)
        + mm(left_high, right_low, dims)
    )


def head_map(heads, width):
    row = lax.broadcasted_iota(jnp.int32, (heads, width), 0)
    lane = lax.broadcasted_iota(jnp.int32, (heads, width), 1)
    span = width // heads
    inside = (lane >= row * span) & (lane < (row + 1) * span)
    return jnp.where(inside, 1.0, 0.0).astype(BF16)


def spread_heads(value, mapping, parts=two):
    return sum(mm(part, mapping, TN) for part in parts(value))


def gather_heads(value, mapping):
    return sum(mm(mapping, part, NT) for part in two(value))


def tri(length, keep):
    row = lax.broadcasted_iota(jnp.int32, (length, length), 0)
    col = lax.broadcasted_iota(jnp.int32, (length, length), 1)
    return jnp.where(keep(row, col), 1.0, 0.0).astype(F32)


def decay_logs(step, rate):
    length = step.shape[1]
    return mm_f32(-(rate * step), tri(length, lambda r, c: r <= c), NN)


def row_sums(value):
    length, width = value.shape
    folded = value[:, :LANES]
    for at in range(LANES, width, LANES):
        folded = folded + value[:, at : at + LANES]
    return jnp.sum(jnp.transpose(folded), axis=0, keepdims=True)


def tree(values):
    values = list(values)
    while len(values) > 1:
        values = [a + b for a, b in zip(values[::2], values[1::2])]
    return values[0]


def last_log_row(logs, mapping_shape):
    heads, width = mapping_shape
    mapping = head_map(heads, width).astype(F32)
    return jnp.sum(mapping * logs[:, -1:], axis=0, keepdims=True)


def carried(index, own_ref, mate_ref, far_refs, state, reverse):
    chip = index // 2
    core = index % 2
    count = len(far_refs) + 1
    logs = []
    for ref in far_refs:
        parts = ref[state : state + ROWS, :].astype(F32)
        logs.append(parts[0:1] + (parts[1:2] + parts[2:3]))
    total = None
    for turn, ref in enumerate(far_refs):
        source = jnp.bitwise_xor(chip, turn + 1)
        log = jnp.zeros_like(logs[0])
        for other in range(1, count):
            middle = jnp.bitwise_xor(chip, other)
            if reverse:
                between = (middle > chip) & (middle < source)
            else:
                between = (middle < chip) & (middle > source)
            log = log + jnp.where(between, logs[other - 1], 0.0)
        wanted = source > chip if reverse else source < chip
        weight = jnp.where(wanted, jnp.exp(log), 0.0)
        part = weight * ref[:state, :].astype(F32)
        total = part if total is None else total + part
    mate = mate_ref[:state, :]
    mate_log = mate_ref[state : state + 1, :]
    behind = core == 0 if reverse else core == 1
    return jnp.where(behind, jnp.exp(mate_log) * total + mate, total)


def state_kernel(step_ref, rate_ref, x_ref, b_ref, out_ref):
    step = step_ref[...]
    heads = step.shape[0]
    width = x_ref.shape[1]
    state = b_ref.shape[1]
    logs = decay_logs(step, rate_ref[...])
    mapping = head_map(heads, width)
    weight = spread_heads(step * jnp.exp(logs[:, -1:] - logs), mapping)
    out_ref[:state, :] = mm_exact_left(b_ref[...], x_ref[...].astype(F32) * weight, TN)
    out_ref[state:, :] = jnp.broadcast_to(last_log_row(logs, mapping.shape), (ROWS, width))


def pair_kernel(reverse, index_ref, own_ref, mate_ref, out_ref):
    state = own_ref.shape[0] - ROWS
    width = own_ref.shape[1]
    core = index_ref[0] % 2
    own_last = core == 0 if reverse else core == 1
    own, mate = own_ref[:state, :], mate_ref[:state, :]
    own_log, mate_log = own_ref[state : state + 1, :], mate_ref[state : state + 1, :]
    second = jnp.where(own_last, own, mate)
    first = jnp.where(own_last, mate, own)
    second_log = jnp.where(own_last, own_log, mate_log)
    out_ref[:state, :] = jnp.exp(second_log) * first + second
    parts = [part.astype(F32) for part in three(own_log + mate_log)]
    row = lax.broadcasted_iota(jnp.int32, (2 * ROWS, width), 0)
    packed = jnp.where(row == 0, parts[0], jnp.where(row == 1, parts[1], parts[2]))
    out_ref[state:, :] = packed


def intra_kernel(step_ref, rate_ref, x_ref, b_ref, c_ref, out_ref, logs_ref, wide_ref):
    step = step_ref[...]
    heads, length = step.shape
    width = x_ref.shape[1]
    span = width // heads
    each = LANES // span
    logs_ref[...] = decay_logs(step, rate_ref[...])
    mapping = head_map(heads, width)
    wide_ref[...] = spread_heads(logs_ref[...], mapping, three)
    scores = mm(c_ref[...], b_ref[...], NT)
    row = lax.broadcasted_iota(jnp.int32, (length, length), 0)
    col = lax.broadcasted_iota(jnp.int32, (length, length), 1)
    scores = jnp.where(row >= col, scores, 0.0)
    lane = lax.broadcasted_iota(jnp.int32, (length, LANES), 1)

    def tile(turn, carry):
        at = pl.multiple_of(turn * LANES, LANES)
        x = x_ref[:, pl.ds(at, LANES)]
        columns = wide_ref[:, pl.ds(at, LANES)]
        result = None
        for one in range(each):
            head = turn * each + one
            later = columns[:, one * span : one * span + 1]
            earlier = logs_ref[pl.ds(head, 1), :]
            table = jnp.exp(jnp.minimum(later - earlier, 0.0))
            mixing = table * scores * step_ref[pl.ds(head, 1), :]
            part = mm_exact_right(mixing, x, NN)
            result = part if one == 0 else jnp.where(lane < one * span, result, part)
        out_ref[:, pl.ds(at, LANES)] = result
        return carry

    lax.fori_loop(0, width // LANES, tile, 0)


def output_kernel(
    index_ref, step_ref, rate_ref, c_ref, z_ref, near_ref, own_ref, mate_ref, *rest
):
    far_refs, (y_ref, u_ref, state_ref, square_ref) = rest[:-4], rest[-4:]
    step = step_ref[...]
    heads = step.shape[0]
    state, width = state_ref.shape
    logs = decay_logs(step, rate_ref[...])
    mapping = head_map(heads, width)
    front = spread_heads(jnp.exp(logs), mapping)
    incoming = carried(index_ref[0], own_ref, mate_ref, far_refs, state, False)
    state_ref[...] = incoming
    y = near_ref[...] + front * mm_exact_left(c_ref[...], incoming, NN)
    y_ref[...] = y
    z = z_ref[...].astype(F32)
    u = y * z * jax.nn.sigmoid(z)
    u_ref[...] = u
    square_ref[...] = jnp.broadcast_to(row_sums(u * u), square_ref.shape)


def arrange_kernel(ratio, up_count, index_ref, *refs):
    place, line = index_ref[0], index_ref[1]
    sources, outs = refs[: 2 * up_count + 1], refs[2 * up_count + 1 :]
    cols = outs[0].shape[1]
    for turn, out_ref in enumerate(outs):
        wanted = jnp.bitwise_xor(place, turn)
        offset = wanted // ratio - line
        at = pl.multiple_of((wanted % ratio) * cols, LANES)
        for slot, source in enumerate(sources):
            @pl.when(offset == slot - up_count)
            def _(out_ref=out_ref, source=source, at=at):
                out_ref[...] = source[:, pl.ds(at, cols)]


def project_kernel(counts, u_ref, gain_ref, square_ref, *refs):
    lefts = refs[: len(counts)]
    weights, (out_ref, stats_ref) = refs[len(counts) : -2], refs[-2:]
    total = None
    at = 0
    for left, count in zip(lefts, counts):
        start = 0
        for weight in weights[at : at + count]:
            rows = weight.shape[0]
            part = mm(left[:, start : start + rows], weight[...], NN)
            total = part if total is None else total + part
            start += rows
        at += count
    out_ref[...] = total
    cross = row_sums(total * gain_ref[...] * u_ref[...])
    row = lax.broadcasted_iota(jnp.int32, stats_ref.shape, 0)
    stats_ref[...] = jnp.where(row == 0, square_ref[...], cross)


def norm_kernel(total_width, step_ref, rate_ref, c_ref, z_ref, y_ref, u_ref, gn_ref, gain_ref, *refs):
    stats_refs, outs = refs[:-5], refs[-5:]
    normed_ref, gates_ref, grad_ref, gain_out_ref, adjoint_ref = outs
    step = step_ref[...]
    heads = step.shape[0]
    width = y_ref.shape[1]
    state = c_ref.shape[1]
    stats = jnp.transpose(tree(ref[...] for ref in stats_refs))
    inv_rms = lax.rsqrt(stats[:, 0:1] / total_width + EPSILON)
    cross = inv_rms * inv_rms * stats[:, 1:2] / total_width
    gain = gain_ref[...]
    z = z_ref[...].astype(F32)
    y = y_ref[...]
    u = u_ref[...]
    gn = gn_ref[...]
    sig = jax.nn.sigmoid(z)
    scaled_u = u * inv_rms
    normed_ref[...] = (scaled_u * gain).astype(BF16)
    gain_out_ref[...] = jnp.broadcast_to(
        jnp.sum(gn * scaled_u, axis=0, keepdims=True), gain_out_ref.shape
    )
    grad_u = inv_rms * (gn * gain - u * cross)
    grad_y = grad_u * z * sig
    grad_ref[...] = grad_y
    gates_ref[...] = (grad_u * y * sig * (1.0 + z * (1.0 - sig))).astype(BF16)
    logs = decay_logs(step, rate_ref[...])
    mapping = head_map(heads, width)
    front = spread_heads(jnp.exp(logs), mapping)
    adjoint_ref[:state, :] = mm_exact_left(c_ref[...], front * grad_y, TN)
    adjoint_ref[state:, :] = jnp.broadcast_to(last_log_row(logs, mapping.shape), (ROWS, width))


def backward_kernel(
    step_ref, rate_ref, x_ref, b_ref, c_ref, grad_ref, state_ref,
    value_ref, keys_ref, q_ref, log_ref,
    logs_ref, wide_ref, wide_step_ref, sum_ref, row_ref, col_ref,
):
    step = step_ref[...]
    heads, length = step.shape
    width = x_ref.shape[1]
    state = b_ref.shape[1]
    span = width // heads
    each = LANES // span
    logs_ref[...] = decay_logs(step, rate_ref[...])
    mapping = head_map(heads, width)
    wide_ref[...] = spread_heads(logs_ref[...], mapping, three)
    wide_step_ref[...] = spread_heads(step, mapping, three)
    scores = mm(b_ref[...], c_ref[...], NT)
    row = lax.broadcasted_iota(jnp.int32, (length, length), 0)
    col = lax.broadcasted_iota(jnp.int32, (length, length), 1)
    keep = col >= row
    lane = lax.broadcasted_iota(jnp.int32, (length, LANES), 1)
    sum_ref[...] = jnp.zeros_like(sum_ref)
    col_ref[...] = jnp.zeros_like(col_ref)

    def tile(turn, carry):
        at = pl.multiple_of(turn * LANES, LANES)
        x = x_ref[:, pl.ds(at, LANES)]
        grad_high, grad_low = two(grad_ref[:, pl.ds(at, LANES)])
        columns = wide_ref[:, pl.ds(at, LANES)]
        steps = wide_step_ref[:, pl.ds(at, LANES)]
        result = None
        for one in range(each):
            head = turn * each + one
            inside = (lane >= one * span) & (lane < (one + 1) * span)
            x_head = jnp.where(inside, x, jnp.zeros_like(x))
            earlier = columns[:, one * span : one * span + 1]
            step_col = steps[:, one * span : one * span + 1]
            later = logs_ref[pl.ds(head, 1), :]
            table = jnp.where(keep, jnp.exp(jnp.minimum(later - earlier, 0.0)), 0.0)
            inner = mm(x_head, grad_high, NT) + mm(x_head, grad_low, NT)
            weighted = table * inner
            product = weighted * scores
            sum_ref[...] += weighted * step_col
            row_ref[pl.ds(head, 1), :] = jnp.sum(product * step_col, axis=0, keepdims=True)
            q = jnp.sum(product, axis=1, keepdims=True)
            col_ref[...] = jnp.where(lane == head, q, col_ref[...])
            high, low = two(table * scores)
            part = mm(high, grad_high, NN) + mm(low, grad_high, NN) + mm(high, grad_low, NN)
            result = part if one == 0 else jnp.where(lane < one * span, result, part)
        value_ref[:, pl.ds(at, LANES)] = result
        return carry

    lax.fori_loop(0, width // LANES, tile, 0)
    incoming = state_ref[...]
    front_grad = spread_heads(jnp.exp(logs_ref[...]), mapping) * grad_ref[...]
    keys_ref[:, :state] = mm_exact_right(sum_ref[...], c_ref[...], NN)
    keys_ref[:, state:] = mm_exact_right(sum_ref[...], b_ref[...], TN) + mm_both(
        front_grad, incoming, NT
    )
    q_near = jnp.transpose(col_ref[...])[:heads, :]
    reach = gather_heads(front_grad * mm_exact_left(c_ref[...], incoming, NN), mapping)
    drive = row_ref[...] - step * q_near + reach
    q_ref[...] = q_near
    log_ref[...] = mm_f32(drive, tri(length, lambda r, c: r >= c), NN)


def final_kernel(
    index_ref, step_ref, rate_ref, x_ref, b_ref, value_ref, q_ref, log_ref, state_ref,
    own_ref, mate_ref, *rest,
):
    far_refs, (inputs_ref, keys_ref, step_out_ref, rate_out_ref) = rest[:-4], rest[-4:]
    step = step_ref[...]
    rate = rate_ref[...]
    heads, length = step.shape
    state, width = state_ref.shape
    logs = decay_logs(step, rate)
    mapping = head_map(heads, width)
    tail = spread_heads(jnp.exp(logs[:, -1:] - logs), mapping)
    wide_step = spread_heads(step, mapping)
    incoming = carried(index_ref[0], own_ref, mate_ref, far_refs, state, True)
    x = x_ref[...].astype(F32)
    reach = tail * mm_exact_left(b_ref[...], incoming, NN)
    inputs_ref[...] = (wide_step * (value_ref[...] + reach)).astype(BF16)
    keys_ref[...] = mm_both(wide_step * tail * x, incoming, NT).astype(keys_ref.dtype)
    far_q = gather_heads(reach * x, mapping)
    through = jnp.sum(incoming * state_ref[...], axis=0, keepdims=True)
    through = gather_heads(jnp.broadcast_to(through, (ROWS, width)), mapping)[:, :1]
    before = mm_f32(step * far_q, tri(length, lambda r, c: r < c), NN)
    log_grad = log_ref[...] + jnp.exp(logs[:, -1:]) * through + before
    step_out_ref[...] = q_ref[...] + far_q - rate * log_grad
    part = -jnp.sum(step * log_grad, axis=1, keepdims=True)
    rate_out_ref[...] = jnp.broadcast_to(part, rate_out_ref.shape)


def weight_kernel(count, *refs):
    lefts, rights, out_ref = refs[:count], refs[count:-1], refs[-1]
    total = None
    for left, right in zip(lefts, rights):
        part = mm(left[...], right[...], TN)
        total = part if total is None else total + part
    out_ref[...] = total


def call(kernel, outs, *args, scratch=(), smem=0):
    specs = [pl.BlockSpec(memory_space=pltpu.SMEM) for _ in range(smem)]
    specs += [pl.BlockSpec(memory_space=pltpu.VMEM) for _ in args[smem:]]
    single = not isinstance(outs, (list, tuple))
    shapes = [outs] if single else list(outs)
    results = pl.pallas_call(
        kernel,
        out_shape=shapes,
        in_specs=specs,
        out_specs=[pl.BlockSpec(memory_space=pltpu.VMEM) for _ in shapes],
        scratch_shapes=list(scratch),
    )(*args)
    return results[0] if single else results


def shape(dims, dtype=F32):
    return jax.ShapeDtypeStruct(tuple(dims), dtype)


def across(value, axis, bits):
    count = lax.axis_size(axis)
    return lax.ppermute(value, axis, [(i, i ^ bits) for i in range(count)])


def shifted(value, axis, by):
    count = lax.axis_size(axis)
    return lax.ppermute(value, axis, [(i, i + by) for i in range(count) if 0 <= i + by < count])


def line_gather(value, axis):
    ups, downs = [], []
    up = down = value
    for _ in range(lax.axis_size(axis) - 1):
        up, down = shifted(up, axis, 1), shifted(down, axis, -1)
        ups.append(up)
        downs.append(down)
    return ups[::-1] + [value] + downs


def cube_gather(value, axis):
    count = lax.axis_size(axis)
    half = value.shape[0] // 2
    found = {0: [value[:half], value[half:]]}
    for bits in range(2, count, 2):
        low = bits & -bits
        high = bits ^ low
        if high == 0:
            found[bits] = [across(piece, axis, bits) for piece in found[0]]
        else:
            found[bits] = [
                across(found[low][0], axis, high),
                across(found[high][1], axis, low),
            ]
    found[1] = [across(value, axis, 1)]
    for bits in range(2, count, 2):
        found[bits + 1] = [across(piece, axis, 1) for piece in found[bits]]
    found[0] = [value]
    return [found[bits] for bits in range(count)]


def xor_sum(value, axis):
    count = lax.axis_size(axis)
    return tree([value] + [across(value, axis, bits) for bits in range(1, count)])


def chip_sum(value, axis):
    count = lax.axis_size(axis)
    value = value + across(value, axis, 1)
    return tree([value] + [across(value, axis, bits) for bits in range(2, count, 2)])


def far_totals(own, mate, index, reverse):
    state, width = own.shape[0] - ROWS, own.shape[1]
    total = call(
        functools.partial(pair_kernel, reverse),
        shape((state + 2 * ROWS, width), F32),
        index, own, mate, smem=1,
    )
    return [across(total, "seq", bits) for bits in range(2, lax.axis_size("seq"), 2)]


def on_device(
    inputs, gates, b_proj, c_proj, step_size, decay_rate, norm_gain, out_weight, grad_out
):
    length, width = inputs.shape
    heads = step_size.shape[0]
    state = b_proj.shape[1]
    places, lines = lax.axis_size("seq"), lax.axis_size("head")
    rows = out_weight.shape[0]
    index = jnp.stack([lax.axis_index("seq"), lax.axis_index("head")]).astype(jnp.int32)
    rate = decay_rate.reshape(heads, 1)
    gain = norm_gain.reshape(1, width)

    weights = cube_gather(out_weight, "seq")
    lines_out = line_gather(grad_out, "head")

    own = call(state_kernel, shape((state + ROWS, width)), step_size, rate, inputs, b_proj)
    mate = across(own, "seq", 1)
    far = far_totals(own, mate, index, False)
    near = call(
        intra_kernel, shape((length, width)), step_size, rate, inputs, b_proj, c_proj,
        scratch=[pltpu.VMEM((heads, length), F32), pltpu.VMEM((length, width), F32)],
    )
    ssd_out, gated, state_in, squares = call(
        output_kernel,
        [shape((length, width)), shape((length, width)), shape((state, width)), shape((ROWS, length))],
        index, step_size, rate, c_proj, gates, near, own, mate, *far, smem=1,
    )
    columns = call(
        functools.partial(arrange_kernel, places // lines, lines - 1),
        [shape((length, rows), BF16)] * places,
        index, *lines_out, smem=1,
    )
    grad_normed, stats = call(
        functools.partial(project_kernel, tuple(len(w) for w in weights)),
        [shape((length, width)), shape((ROWS, length))],
        gated, gain, squares, *columns, *[piece for w in weights for piece in w],
    )
    all_stats = [stats] + [across(stats, "head", bits) for bits in range(1, lines)]
    normed, grad_gates, grad_y, gain_part, back_own = call(
        functools.partial(norm_kernel, width * lines),
        [
            shape((length, width), BF16), shape((length, width), BF16), shape((length, width)),
            shape((ROWS, width)), shape((state + ROWS, width)),
        ],
        step_size, rate, c_proj, gates, ssd_out, gated, grad_normed, gain, *all_stats,
    )
    back_mate = across(back_own, "seq", 1)
    back_far = far_totals(back_own, back_mate, index, True)
    value_near, keys_near, q_near, log_near = call(
        backward_kernel,
        [shape((length, width)), shape((length, 2 * state)), shape((heads, length)), shape((heads, length))],
        step_size, rate, inputs, b_proj, c_proj, grad_y, state_in,
        scratch=[
            pltpu.VMEM((heads, length), F32), pltpu.VMEM((length, width), F32),
            pltpu.VMEM((length, width), F32), pltpu.VMEM((length, length), F32),
            pltpu.VMEM((heads, length), F32), pltpu.VMEM((length, LANES), F32),
        ],
    )
    grad_inputs, keys_far, grad_step, rate_part = call(
        final_kernel,
        [
            shape((length, width), BF16), shape((length, state), BF16),
            shape((heads, length)), shape((heads, LANES)),
        ],
        index, step_size, rate, inputs, b_proj, value_near, q_near, log_near, state_in,
        back_own, back_mate, *back_far, smem=1,
    )
    near_sum = xor_sum(keys_near, "head")
    far_sum = tree(
        part.astype(F32)
        for part in [keys_far] + [across(keys_far, "head", bits) for bits in range(1, lines)]
    )
    grad_b = near_sum[:, :state] + far_sum
    grad_c = near_sum[:, state:]
    grad_gain = chip_sum(gain_part, "seq")[0]
    grad_rate = chip_sum(rate_part, "seq")[:, 0]

    swapped = [columns[0]] + [across(columns[bits], "seq", bits) for bits in range(1, places)]
    gathered = [normed] + [across(normed, "seq", bits) for bits in range(1, places)]
    grad_weight = call(
        functools.partial(weight_kernel, places), shape((rows, width)), *swapped, *gathered
    )
    return (grad_inputs, grad_gates, grad_b, grad_c, grad_step, grad_rate, grad_gain, grad_weight)


def solution(mesh):
    in_specs = (
        P("seq", "head"),
        P("seq", "head"),
        P("seq", None),
        P("seq", None),
        P("head", "seq"),
        P("head"),
        P("head"),
        P("seq", "head"),
        P("seq", "head"),
    )
    out_specs = (
        P("seq", "head"),
        P("seq", "head"),
        P("seq", None),
        P("seq", None),
        P("head", "seq"),
        P("head"),
        P("head"),
        P("seq", "head"),
    )
    return jax.shard_map(
        on_device, mesh=mesh, in_specs=in_specs, out_specs=out_specs, check_vma=False
    )
```

```python
import functools
import math

import jax
import jax.numpy as jnp
from jax import lax
from jax.experimental import pallas as pl
from jax.experimental.pallas import tpu as pltpu
from jax.sharding import PartitionSpec as P


EPSILON = 1e-05
F32 = jnp.float32
BF16 = jnp.bfloat16
LANES = 128
ROWS = 8
NN = ((1,), (0,))
NT = ((1,), (1,))
TN = ((0,), (0,))
HIGHEST = lax.Precision.HIGHEST
SPARE_BYTES = 10 << 20
FLOPS_PER_US = 500_000_000


def mm(left, right, dims):
    return lax.dot_general(left, right, (dims, ((), ())), preferred_element_type=F32)


def mm_f32(left, right, dims):
    return lax.dot_general(
        left, right, (dims, ((), ())), precision=HIGHEST, preferred_element_type=F32
    )


def two(value):
    high = value.astype(BF16)
    return high, (value - high.astype(F32)).astype(BF16)


def three(value):
    high = value.astype(BF16)
    rest = value - high.astype(F32)
    middle = rest.astype(BF16)
    return high, middle, (rest - middle.astype(F32)).astype(BF16)


def mm_exact_left(left, right, dims):
    high, low = two(right)
    return mm(left, high, dims) + mm(left, low, dims)


def mm_exact_right(left, right, dims):
    high, low = two(left)
    return mm(high, right, dims) + mm(low, right, dims)


def mm_both(left, right, dims):
    left_high, left_low = two(left)
    right_high, right_low = two(right)
    return (
        mm(left_high, right_high, dims)
        + mm(left_low, right_high, dims)
        + mm(left_high, right_low, dims)
    )


def head_map(heads, width):
    row = lax.broadcasted_iota(jnp.int32, (heads, width), 0)
    lane = lax.broadcasted_iota(jnp.int32, (heads, width), 1)
    span = width // heads
    inside = (lane >= row * span) & (lane < (row + 1) * span)
    return jnp.where(inside, 1.0, 0.0).astype(BF16)


def spread_heads(value, mapping, parts=two):
    return sum(mm(part, mapping, TN) for part in parts(value))


def gather_heads(value, mapping):
    return sum(mm(mapping, part, NT) for part in two(value))


def tri(length, keep):
    row = lax.broadcasted_iota(jnp.int32, (length, length), 0)
    col = lax.broadcasted_iota(jnp.int32, (length, length), 1)
    return jnp.where(keep(row, col), 1.0, 0.0).astype(F32)


def decay_logs(step, rate):
    length = step.shape[1]
    return mm_f32(-(rate * step), tri(length, lambda r, c: r <= c), NN)


def row_sums(value):
    _, width = value.shape
    folded = value[:, :LANES]
    for at in range(LANES, width, LANES):
        folded = folded + value[:, at : at + LANES]
    return jnp.sum(jnp.transpose(folded), axis=0, keepdims=True)


def tree(values):
    values = list(values)
    while len(values) > 1:
        values = [a + b for a, b in zip(values[::2], values[1::2])]
    return values[0]


def last_log_row(logs, mapping_shape):
    heads, width = mapping_shape
    mapping = head_map(heads, width).astype(F32)
    return jnp.sum(mapping * logs[:, -1:], axis=0, keepdims=True)


def far_state(index, far_refs, state, reverse):
    chip = index // 2
    count = len(far_refs) + 1
    logs = []
    for ref in far_refs:
        parts = ref[state : state + ROWS, :].astype(F32)
        logs.append(parts[0:1] + (parts[1:2] + parts[2:3]))
    total = None
    for turn, ref in enumerate(far_refs):
        source = jnp.bitwise_xor(chip, turn + 1)
        log = jnp.zeros_like(logs[0])
        for other in range(1, count):
            middle = jnp.bitwise_xor(chip, other)
            if reverse:
                between = (middle > chip) & (middle < source)
            else:
                between = (middle < chip) & (middle > source)
            log = log + jnp.where(between, logs[other - 1], 0.0)
        wanted = source > chip if reverse else source < chip
        weight = jnp.where(wanted, jnp.exp(log), 0.0)
        part = weight * ref[:state, :].astype(F32)
        total = part if total is None else total + part
    return total


def carried(index, mate_ref, half_ref, other_ref, reverse):
    core = index % 2
    state = half_ref.shape[0]
    half, other = half_ref[...], other_ref[...]
    total = jnp.concatenate(
        [jnp.where(core == 0, half, other), jnp.where(core == 0, other, half)], axis=1
    )
    behind = core == 0 if reverse else core == 1
    mate_log = mate_ref[state : state + 1, :]
    return jnp.where(behind, jnp.exp(mate_log) * total + mate_ref[:state, :], total)


def state_kernel(step_ref, rate_ref, x_ref, b_ref, out_ref):
    step = step_ref[...]
    heads = step.shape[0]
    width = x_ref.shape[1]
    state = b_ref.shape[1]
    logs = decay_logs(step, rate_ref[...])
    mapping = head_map(heads, width)
    weight = spread_heads(step * jnp.exp(logs[:, -1:] - logs), mapping)
    out_ref[:state, :] = mm_exact_left(b_ref[...], x_ref[...].astype(F32) * weight, TN)
    out_ref[state:, :] = jnp.broadcast_to(last_log_row(logs, mapping.shape), (ROWS, width))


def pair_kernel(reverse, index_ref, own_ref, mate_ref, out_ref):
    state = own_ref.shape[0] - ROWS
    width = out_ref.shape[1]
    core = index_ref[0] % 2
    own_last = core == 0 if reverse else core == 1
    at = pl.multiple_of(core * width, LANES)
    own, mate = own_ref[:, pl.ds(at, width)], mate_ref[:, pl.ds(at, width)]
    second = jnp.where(own_last, own, mate)
    first = jnp.where(own_last, mate, own)
    second_log = second[state : state + 1]
    total = jnp.exp(second_log) * first[:state] + second[:state]
    out_ref[:state, :] = total.astype(out_ref.dtype)
    parts = [part.astype(F32) for part in three(second_log + first[state : state + 1])]
    row = lax.broadcasted_iota(jnp.int32, (2 * ROWS, width), 0)
    packed = jnp.where(row == 0, parts[0], jnp.where(row == 1, parts[1], parts[2]))
    out_ref[state:, :] = packed.astype(out_ref.dtype)


def merge_kernel(reverse, index_ref, *refs):
    far_refs, out_ref = refs[:-1], refs[-1]
    out_ref[...] = far_state(index_ref[0], far_refs, out_ref.shape[0], reverse)


def intra_kernel(step_ref, rate_ref, x_ref, b_ref, c_ref, out_ref, logs_ref, wide_ref):
    step = step_ref[...]
    heads, length = step.shape
    width = x_ref.shape[1]
    span = width // heads
    each = LANES // span
    logs_ref[...] = decay_logs(step, rate_ref[...])
    mapping = head_map(heads, width)
    wide_ref[...] = spread_heads(logs_ref[...], mapping, three)
    scores = mm(c_ref[...], b_ref[...], NT)
    row = lax.broadcasted_iota(jnp.int32, (length, length), 0)
    col = lax.broadcasted_iota(jnp.int32, (length, length), 1)
    scores = jnp.where(row >= col, scores, 0.0)
    lane = lax.broadcasted_iota(jnp.int32, (length, LANES), 1)

    def tile(turn, carry):
        at = pl.multiple_of(turn * LANES, LANES)
        x = x_ref[:, pl.ds(at, LANES)]
        columns = wide_ref[:, pl.ds(at, LANES)]
        result = None
        for one in range(each):
            head = turn * each + one
            later = columns[:, one * span : one * span + 1]
            earlier = logs_ref[pl.ds(head, 1), :]
            table = jnp.exp(jnp.minimum(later - earlier, 0.0))
            mixing = table * scores * step_ref[pl.ds(head, 1), :]
            part = mm_exact_right(mixing, x, NN)
            result = part if one == 0 else jnp.where(lane < one * span, result, part)
        out_ref[:, pl.ds(at, LANES)] = result
        return carry

    lax.fori_loop(0, width // LANES, tile, 0)


def output_kernel(
    index_ref, step_ref, rate_ref, c_ref, z_ref, near_ref, mate_ref, half_ref, other_ref,
    y_ref, u_ref, state_ref, square_ref,
):
    step = step_ref[...]
    heads = step.shape[0]
    _, width = state_ref.shape
    logs = decay_logs(step, rate_ref[...])
    mapping = head_map(heads, width)
    front = spread_heads(jnp.exp(logs), mapping)
    incoming = carried(index_ref[0], mate_ref, half_ref, other_ref, False)
    state_ref[...] = incoming
    y = near_ref[...] + front * mm_exact_left(c_ref[...], incoming, NN)
    y_ref[...] = y
    z = z_ref[...].astype(F32)
    u = y * z * jax.nn.sigmoid(z)
    u_ref[...] = u
    square_ref[...] = jnp.broadcast_to(row_sums(u * u), square_ref.shape)


def copy_columns(sources, wanted, out_ref, at, cols):
    for slot, source in enumerate(sources):

        @pl.when(wanted == slot)
        def _(source=source):
            out_ref[...] = source[:, pl.ds(at, cols)]


def pick(core, pair):
    return pair[0] if pair[0] == pair[1] else jnp.where(core == 0, pair[0], pair[1])


def arrange_kernel(offsets, ratio, sources, index_ref, *refs):
    place, line = index_ref[0], index_ref[1]
    for bits, out_ref in zip(offsets, refs[sources:]):
        cols = out_ref.shape[1]
        wanted = (jnp.bitwise_xor(place, bits) // 2) * 2
        at = pl.multiple_of((wanted % ratio) * (cols // 2), LANES)
        copy_columns(refs[:sources], jnp.bitwise_xor(wanted // ratio, line), out_ref, at, cols)


def project_kernel(offsets, sources, index_ref, u_ref, gain_ref, square_ref, *refs):
    place, line = index_ref[0], index_ref[1]
    core = place % 2
    slots, weights = refs[:sources], refs[sources : sources + len(offsets)]
    out_ref, stats_ref, full_ref = refs[sources + len(offsets) :]
    cols = slots[0].shape[1]
    for turn in range(sources):
        block = full_ref.at[:, turn * cols : (turn + 1) * cols]
        copy_columns(slots, jnp.bitwise_xor(turn, line), block, 0, cols)
    total = None
    for pair, weight in zip(offsets, weights):
        rows = weight.shape[0]
        wanted = jnp.bitwise_xor(place, pick(core, pair))
        left = full_ref[:, pl.ds(pl.multiple_of(wanted * rows, LANES), rows)]
        part = mm(left, weight[...], NN)
        total = part if total is None else total + part
    out_ref[...] = total
    cross = row_sums(total * gain_ref[...] * u_ref[...])
    row = lax.broadcasted_iota(jnp.int32, stats_ref.shape, 0)
    stats_ref[...] = jnp.where(row == 0, square_ref[...], cross)


def norm_kernel(total_width, step_ref, rate_ref, c_ref, z_ref, y_ref, u_ref, gn_ref, gain_ref, *refs):
    stats_refs, outs = refs[:-5], refs[-5:]
    normed_ref, gates_ref, grad_ref, gain_out_ref, adjoint_ref = outs
    step = step_ref[...]
    heads = step.shape[0]
    width = y_ref.shape[1]
    state = c_ref.shape[1]
    stats = jnp.transpose(tree(ref[...] for ref in stats_refs))
    inv_rms = lax.rsqrt(stats[:, 0:1] / total_width + EPSILON)
    cross = inv_rms * inv_rms * stats[:, 1:2] / total_width
    gain = gain_ref[...]
    z = z_ref[...].astype(F32)
    y = y_ref[...]
    u = u_ref[...]
    gn = gn_ref[...]
    sig = jax.nn.sigmoid(z)
    scaled_u = u * inv_rms
    normed_ref[...] = (scaled_u * gain).astype(BF16)
    gain_out_ref[...] = jnp.broadcast_to(
        jnp.sum(gn * scaled_u, axis=0, keepdims=True), gain_out_ref.shape
    )
    grad_u = inv_rms * (gn * gain - u * cross)
    grad_y = grad_u * z * sig
    grad_ref[...] = grad_y
    gates_ref[...] = (grad_u * y * sig * (1.0 + z * (1.0 - sig))).astype(BF16)
    logs = decay_logs(step, rate_ref[...])
    mapping = head_map(heads, width)
    front = spread_heads(jnp.exp(logs), mapping)
    adjoint_ref[:state, :] = mm_exact_left(c_ref[...], front * grad_y, TN)
    adjoint_ref[state:, :] = jnp.broadcast_to(last_log_row(logs, mapping.shape), (ROWS, width))


def backward_kernel(
    step_ref, rate_ref, x_ref, b_ref, c_ref, grad_ref, state_ref,
    value_ref, keys_ref, q_ref, log_ref,
    logs_ref, wide_ref, wide_step_ref, sum_ref, row_ref, col_ref,
):
    step = step_ref[...]
    heads, length = step.shape
    width = x_ref.shape[1]
    state = b_ref.shape[1]
    span = width // heads
    each = LANES // span
    logs_ref[...] = decay_logs(step, rate_ref[...])
    mapping = head_map(heads, width)
    wide_ref[...] = spread_heads(logs_ref[...], mapping, three)
    wide_step_ref[...] = spread_heads(step, mapping, three)
    scores = mm(b_ref[...], c_ref[...], NT)
    row = lax.broadcasted_iota(jnp.int32, (length, length), 0)
    col = lax.broadcasted_iota(jnp.int32, (length, length), 1)
    keep = col >= row
    lane = lax.broadcasted_iota(jnp.int32, (length, LANES), 1)
    sum_ref[...] = jnp.zeros_like(sum_ref)
    col_ref[...] = jnp.zeros_like(col_ref)

    def tile(turn, carry):
        at = pl.multiple_of(turn * LANES, LANES)
        x = x_ref[:, pl.ds(at, LANES)]
        grad_high, grad_low = two(grad_ref[:, pl.ds(at, LANES)])
        columns = wide_ref[:, pl.ds(at, LANES)]
        steps = wide_step_ref[:, pl.ds(at, LANES)]
        result = None
        for one in range(each):
            head = turn * each + one
            inside = (lane >= one * span) & (lane < (one + 1) * span)
            x_head = jnp.where(inside, x, jnp.zeros_like(x))
            earlier = columns[:, one * span : one * span + 1]
            step_col = steps[:, one * span : one * span + 1]
            later = logs_ref[pl.ds(head, 1), :]
            table = jnp.where(keep, jnp.exp(jnp.minimum(later - earlier, 0.0)), 0.0)
            inner = mm(x_head, grad_high, NT) + mm(x_head, grad_low, NT)
            weighted = table * inner
            product = weighted * scores
            sum_ref[...] += weighted * step_col
            row_ref[pl.ds(head, 1), :] = jnp.sum(product * step_col, axis=0, keepdims=True)
            q = jnp.sum(product, axis=1, keepdims=True)
            col_ref[...] = jnp.where(lane == head, q, col_ref[...])
            high, low = two(table * scores)
            part = mm(high, grad_high, NN) + mm(low, grad_high, NN) + mm(high, grad_low, NN)
            result = part if one == 0 else jnp.where(lane < one * span, result, part)
        value_ref[:, pl.ds(at, LANES)] = result
        return carry

    lax.fori_loop(0, width // LANES, tile, 0)
    incoming = state_ref[...]
    front_grad = spread_heads(jnp.exp(logs_ref[...]), mapping) * grad_ref[...]
    keys_ref[:, :state] = mm_exact_right(sum_ref[...], c_ref[...], NN).astype(keys_ref.dtype)
    queries = mm_exact_right(sum_ref[...], b_ref[...], TN) + mm_both(front_grad, incoming, NT)
    keys_ref[:, state:] = queries.astype(keys_ref.dtype)
    q_near = jnp.transpose(col_ref[...])[:heads, :]
    reach = gather_heads(front_grad * mm_exact_left(c_ref[...], incoming, NN), mapping)
    drive = row_ref[...] - step * q_near + reach
    q_ref[...] = q_near
    log_ref[...] = mm_f32(drive, tri(length, lambda r, c: r >= c), NN)


def final_kernel(
    index_ref, step_ref, rate_ref, x_ref, b_ref, value_ref, q_ref, log_ref, state_ref,
    gain_ref, mate_ref, half_ref, other_ref,
    inputs_ref, keys_ref, step_out_ref, sums_ref,
):
    step = step_ref[...]
    rate = rate_ref[...]
    heads, length = step.shape
    _, width = state_ref.shape
    logs = decay_logs(step, rate)
    mapping = head_map(heads, width)
    tail = spread_heads(jnp.exp(logs[:, -1:] - logs), mapping)
    wide_step = spread_heads(step, mapping)
    incoming = carried(index_ref[0], mate_ref, half_ref, other_ref, True)
    x = x_ref[...].astype(F32)
    reach = tail * mm_exact_left(b_ref[...], incoming, NN)
    inputs_ref[...] = (wide_step * (value_ref[...] + reach)).astype(BF16)
    keys_ref[...] = mm_both(wide_step * tail * x, incoming, NT).astype(keys_ref.dtype)
    far_q = gather_heads(reach * x, mapping)
    through = jnp.sum(incoming * state_ref[...], axis=0, keepdims=True)
    through = gather_heads(jnp.broadcast_to(through, (ROWS, width)), mapping)[:, :1]
    before = mm_f32(step * far_q, tri(length, lambda r, c: r < c), NN)
    log_grad = log_ref[...] + jnp.exp(logs[:, -1:]) * through + before
    step_out_ref[...] = q_ref[...] + far_q - rate * log_grad
    part = -jnp.sum(step * log_grad, axis=1, keepdims=True)
    row = lax.broadcasted_iota(jnp.int32, (heads, LANES), 0)
    lane = lax.broadcasted_iota(jnp.int32, (heads, LANES), 1)
    part = jnp.sum(jnp.where(row == lane, part, 0.0), axis=0, keepdims=True)
    sums_ref[:, :width] = gain_ref[...]
    sums_ref[:, width:] = jnp.broadcast_to(part, (ROWS, LANES))


def weight_kernel(mine, offsets, index_ref, *refs):
    core = index_ref[0] % 2
    count = len(offsets)
    rights, lefts, out_ref = refs[:count], refs[count : 2 * count], refs[-1]
    rows = out_ref.shape[0]
    side = core if mine else 1 - core
    at = pl.multiple_of(side * rows, LANES)
    total = None
    for pair, right in zip(offsets, rights):
        first, second = lefts[pair[0] // 2], lefts[pair[1] // 2]
        left = first[:, pl.ds(at, rows)]
        if pair[0] != pair[1]:
            left = jnp.where(core == 0, left, second[:, pl.ds(at, rows)])
        part = mm(left, right[...], TN)
        total = part if total is None else total + part
    out_ref[...] = total.astype(out_ref.dtype)


def size(value):
    return math.prod(value.shape) * value.dtype.itemsize


def call(kernel, outs, *args, scratch=(), smem=0, cost=1.0):
    specs = [pl.BlockSpec(memory_space=pltpu.SMEM) for _ in range(smem)]
    specs += [pl.BlockSpec(memory_space=pltpu.VMEM) for _ in args[smem:]]
    single = not isinstance(outs, (list, tuple))
    shapes = [outs] if single else list(outs)
    held = sum(size(value) for value in [*args, *shapes, *scratch])
    results = pl.pallas_call(
        kernel,
        out_shape=shapes,
        in_specs=specs,
        out_specs=[pl.BlockSpec(memory_space=pltpu.VMEM) for _ in shapes],
        scratch_shapes=list(scratch),
        compiler_params=pltpu.CompilerParams(vmem_limit_bytes=held + SPARE_BYTES),
        cost_estimate=pl.CostEstimate(
            flops=int(cost * FLOPS_PER_US), transcendentals=0, bytes_accessed=held
        ),
    )(*args)
    return results[0] if single else results


def shape(dims, dtype=F32):
    return jax.ShapeDtypeStruct(tuple(dims), dtype)


def across(value, axis, bits, odd_bits=None):
    odd_bits = bits if odd_bits is None else odd_bits
    count = lax.axis_size(axis)
    return lax.ppermute(
        value, axis, [(i, i ^ (odd_bits if i % 2 else bits)) for i in range(count)]
    )


def line_gather(value, axis):
    count = lax.axis_size(axis)
    if count == 4:
        last = across(value, axis, 3)
        near = across(value, axis, 1)
        return [value, near, across(last, axis, 1), last]
    return [value] + [across(value, axis, bits) for bits in range(1, count)]


def chip_gather(value, axis):
    count = lax.axis_size(axis)
    if count == 8:
        first = across(value, axis, 2, 4)
        second = across(value, axis, 4, 2)
        third = across(first, axis, 4, 2)
        return [value, first, second, third], [(0, 0), (2, 4), (4, 2), (6, 6)]
    steps = range(0, count, 2)
    blocks = [value] + [across(value, axis, bits) for bits in steps[1:]]
    return blocks, [(bits, bits) for bits in steps]


def mate_gather(blocks, offsets, axis):
    return (
        blocks + [across(block, axis, 1) for block in blocks],
        offsets + [(1 ^ second, 1 ^ first) for first, second in offsets],
    )


def chip_sum(value, axis):
    count = lax.axis_size(axis)
    value = value + across(value, axis, 1)
    return tree([value] + [across(value, axis, bits) for bits in range(2, count, 2)])


def far_halves(own, mate, index, reverse, dtype):
    state, width = own.shape[0] - ROWS, own.shape[1] // 2
    total = call(
        functools.partial(pair_kernel, reverse),
        shape((state + 2 * ROWS, width), dtype),
        index, own, mate, smem=1,
    )
    far = [across(total, "seq", bits) for bits in range(2, lax.axis_size("seq"), 2)]
    half = call(
        functools.partial(merge_kernel, reverse), shape((state, width)), index, *far, smem=1
    )
    return total, half, across(half, "seq", 1)


def layer(
    inputs, gates, b_proj, c_proj, step_size, decay_rate, norm_gain, out_weight, grad_out
):
    length, width = inputs.shape
    heads = step_size.shape[0]
    state = b_proj.shape[1]
    places, lines = lax.axis_size("seq"), lax.axis_size("head")
    rows = out_weight.shape[0]
    index = jnp.stack([lax.axis_index("seq"), lax.axis_index("head")]).astype(jnp.int32)
    rate = decay_rate.reshape(heads, 1)
    gain = norm_gain.reshape(1, width)

    own = call(state_kernel, shape((state + ROWS, width)), step_size, rate, inputs, b_proj)
    chips, chip_bits = chip_gather(out_weight, "seq")
    slots = line_gather(grad_out, "head")
    mate = across(own, "seq", 1)
    _, half, other = far_halves(own, mate, index, False, F32)
    weights, weight_bits = mate_gather(chips, chip_bits, "seq")
    near = call(
        intra_kernel, shape((length, width)), step_size, rate, inputs, b_proj, c_proj,
        scratch=[pltpu.VMEM((heads, length), F32), pltpu.VMEM((length, width), F32)],
    )
    ssd_out, gated, state_in, squares = call(
        output_kernel,
        [shape((length, width)), shape((length, width)), shape((state, width)), shape((ROWS, length))],
        index, step_size, rate, c_proj, gates, near, mate, half, other, smem=1,
    )
    grad_normed, stats = call(
        functools.partial(project_kernel, weight_bits, len(slots)),
        [shape((length, width)), shape((ROWS, length))],
        index, gated, gain, squares, *slots, *weights, smem=1,
        scratch=[pltpu.VMEM((length, width * lines), BF16)],
    )
    all_stats = [stats] + [across(stats, "head", bits) for bits in range(1, lines)]
    steps = range(0, places, 2)
    pieces = call(
        functools.partial(arrange_kernel, steps, places // lines, len(slots)),
        [shape((length, 2 * rows), BF16)] * len(steps),
        index, *slots, smem=1,
    )
    swapped = [pieces[0]] + [
        across(piece, "seq", bits) for piece, bits in zip(pieces[1:], steps[1:])
    ]
    normed, grad_gates, grad_y, gain_part, back_own = call(
        functools.partial(norm_kernel, width * lines),
        [
            shape((length, width), BF16), shape((length, width), BF16), shape((length, width)),
            shape((ROWS, width)), shape((state + ROWS, width)),
        ],
        step_size, rate, c_proj, gates, ssd_out, gated, grad_normed, gain, *all_stats,
    )
    back_mate = across(back_own, "seq", 1)
    back_total, back_half, back_other = far_halves(back_own, back_mate, index, True, BF16)
    normed, grad_y, _ = lax.optimization_barrier((normed, grad_y, back_total))
    gathered, gathered_bits = chip_gather(normed, "seq")
    value_near, keys_near, q_near, log_near = call(
        backward_kernel,
        [shape((length, width)), shape((length, 2 * state), BF16), shape((heads, length)), shape((heads, length))],
        step_size, rate, inputs, b_proj, c_proj, grad_y, state_in,
        scratch=[
            pltpu.VMEM((heads, length), F32), pltpu.VMEM((length, width), F32),
            pltpu.VMEM((length, width), F32), pltpu.VMEM((length, length), F32),
            pltpu.VMEM((heads, length), F32), pltpu.VMEM((length, LANES), F32),
        ],
    )
    parts = [keys_near] + [across(keys_near, "head", bits) for bits in range(1, lines)]
    near_sum = tree(part.astype(F32) for part in parts)
    grad_inputs, keys_far, grad_step, sums = call(
        final_kernel,
        [
            shape((length, width), BF16), shape((length, state), BF16),
            shape((heads, length)), shape((ROWS, width + LANES)),
        ],
        index, step_size, rate, inputs, b_proj, value_near, q_near, log_near, state_in,
        gain_part, back_mate, back_half, back_other, smem=1,
    )
    parts = [keys_far] + [across(keys_far, "head", bits) for bits in range(1, lines)]
    far_sum = tree(part.astype(F32) for part in parts)
    grad_b = near_sum[:, :state] + far_sum
    grad_c = near_sum[:, state:]
    sums = chip_sum(sums, "seq")[0]
    grad_gain, grad_rate = sums[:width], sums[width : width + heads]

    gathered, _ = lax.optimization_barrier((gathered, grad_step))

    def product(mine, dtype):
        return call(
            functools.partial(weight_kernel, mine, gathered_bits), shape((rows, width), dtype),
            index, *gathered, *swapped, smem=1,
        )

    grad_weight = product(True, F32) + across(product(False, BF16), "seq", 1).astype(F32)
    return (grad_inputs, grad_gates, grad_b, grad_c, grad_step, grad_rate, grad_gain, grad_weight)


def solution(mesh):
    in_specs = (
        P("seq", "head"),
        P("seq", "head"),
        P("seq", None),
        P("seq", None),
        P("head", "seq"),
        P("head"),
        P("head"),
        P("seq", "head"),
        P("seq", "head"),
    )
    out_specs = (
        P("seq", "head"),
        P("seq", "head"),
        P("seq", None),
        P("seq", None),
        P("head", "seq"),
        P("head"),
        P("head"),
        P("seq", "head"),
    )
    return jax.shard_map(layer, mesh=mesh, in_specs=in_specs, out_specs=out_specs, check_vma=False)
```
